32 devices in a mesh: groups: 1, expert: 16 (over z, y, x), replica: 2 (over core).
Axes of the slice: x: 2, y: 2, z: 4, core: 2. Of those that a mesh axis runs over, the one named last changes fastest.
Arguments:
- queries: bfloat16 [128, 8192], P(('groups', 'expert', 'replica')), may hold values from -250 to 250
- token_keys: bfloat16 [128, 512], P(('groups', 'expert', 'replica')), may hold values from -6 to 6
- token_values: bfloat16 [128, 512], P(('groups', 'expert', 'replica')), may hold values from -6 to 6
- stored_keys: bfloat16 [128, 256, 512], P(('groups', 'expert', 'replica')), may hold values from -7 to 7
- stored_values: bfloat16 [128, 256, 512], P(('groups', 'expert', 'replica')), may hold values from -6 to 6
- kv_len: int32 [128], P(('groups', 'expert', 'replica')), may hold values from 2 to 256, as said below
- residual: bfloat16 [128, 4096], P(('groups', 'expert', 'replica')), may hold values from -6 to 6
- out_weight: bfloat16 [8192, 4096], P(('expert', 'replica')), may hold values from -0.1875 to 0.1875
- norm_gain: bfloat16 [4096], replicated, may hold values from 0.25 to 1.75
- expert_ids: int32 [128, 8], P(('groups', 'expert')), may hold values from 0 to 15, all different within a row; in each aligned block of 8 rows (0 to 7, 8 to 15, ...) at most 4 rows name the same one
- route_weight: float32 [128, 8], P(('groups', 'expert')), may hold values from 0.05 to 1
- w_gate: bfloat16 [16, 4096, 768], P('expert', None, 'replica'), may hold values from -0.09375 to 0.09375
- w_up: bfloat16 [16, 4096, 768], P('expert', None, 'replica'), may hold values from -0.09375 to 0.09375
- w_down: bfloat16 [16, 768, 4096], P('expert', 'replica'), may hold values from -0.4375 to 0.4375
Outputs:
- updated: bfloat16 [128, 4096], P(('groups', 'expert', 'replica'))
The draws below stay inside these ranges and needn't reach their ends.
Inputs may be any that keep to these rules, and one draw needn't show every extreme that they name: `kv_len`: at least 2; some sequence uses all 256 positions. `expert_ids`: each token names 8 different experts; in each aligned block of 8 tokens no expert is named by more than 4 tokens, and some block reaches it.
All inputs are finite; a program needn't handle non-finite values.
Results may differ from the reference program's by a relative error of at most 0.01.
Values may be sent and summed in bfloat16 or wider, within the bound.
A program may use at most 64 MiB of HBM per device.

```python
import math
import jax
import jax.numpy as jnp
import numpy as np
from jax import lax

D = 4096
QUERY_HEADS = 64
KEY_VALUE_HEADS = 4
HEAD_WIDTH = 128
FF = 768
TOPK = 8
SEQ_DEV = 4
CACHE_POSITIONS = 256
EXPERTS = 16
SEQUENCE_TOTAL = 128
MOST = 4
N_EXPERT = 16
N_REPLICA = 2


def key_lookup(key):
    return jnp.clip(jax.random.normal(jax.random.fold_in(key, 11), (SEQUENCE_TOTAL, CACHE_POSITIONS, KEY_VALUE_HEADS * HEAD_WIDTH), jnp.float32), -6.0, 6.0)


def draw_queries(key, part):
    base = jnp.clip(jax.random.normal(jax.random.fold_in(key, 5), (SEQUENCE_TOTAL, QUERY_HEADS * HEAD_WIDTH), jnp.float32), -6.0, 6.0)
    return base.astype(jnp.bfloat16)


def draw_stored_keys(key, part):
    table = key_lookup(key)
    return table.astype(jnp.bfloat16)


def draw_kv_len(key, part):
    lengths = jax.random.randint(jax.random.fold_in(key, 3), (SEQUENCE_TOTAL,), 2, CACHE_POSITIONS + 1, jnp.int32)
    chosen = jax.random.randint(jax.random.fold_in(key, 4), (), 0, SEQUENCE_TOTAL, jnp.int32)
    return jnp.where(jnp.arange(SEQUENCE_TOTAL, dtype=jnp.int32) == chosen, CACHE_POSITIONS, lengths).astype(jnp.int32)


def shard_levels(own_key, shape, cuts, least, high):
    gain, own = 1.0, jax.random.fold_in(own_key, 6)
    for dim, parts in cuts:
        heights = jnp.exp(jax.random.uniform(jax.random.fold_in(own, dim), (parts,), jnp.float32, least / len(cuts), high / len(cuts)))
        gain = gain * jnp.repeat(heights, shape[dim] // parts).reshape([-1 if axis == dim else 1 for axis in range(len(shape))])
    return gain


def shared_out(own_key, own, number, rows, number_of, top, most, slope):
    ranking = jax.random.permutation(own_key, number_of)
    heavy_load, common = portions_of(number_of, rows * top, most, slope, True), portions_of(number_of, rows * top, most, slope, False)
    places = jnp.arange(number_of)

    def named(tallies, turn):
        used = int((tallies > 0).sum())
        fixed = max(1, used // 4)
        shifted = fixed + (places - fixed + turn * (used - fixed)) % max(1, number_of - fixed)
        return jnp.zeros((number_of,), jnp.int32).at[ranking[jnp.where(places < fixed, places, shifted)]].set(jnp.asarray(tallies, jnp.int32))

    tallies = jnp.where(number % 4 == 0, named(heavy_load, number // 4), named(common, number - number // 4 - 1))
    mixed = jax.random.permutation(jax.random.fold_in(own, 3), number_of)
    donor, receiver = mixed[0:number_of // 2 * 2:2], mixed[1:number_of // 2 * 2:2]
    margin = jnp.minimum(tallies[donor] - 1, most - tallies[receiver]) // 2
    margin = jnp.where((donor == ranking[0]) | (receiver == ranking[0]) | (tallies[receiver] == 0), 0, jnp.maximum(margin, 0))
    shifted = jax.random.randint(jax.random.fold_in(own, 4), (number_of // 2,), 0, 1 << 20) % (margin + 1)
    tallies = tallies.at[donor].add(-shifted).at[receiver].add(shifted)
    items = jnp.searchsorted(jnp.cumsum(tallies), jnp.arange(rows * top), side="right").astype(jnp.int32)
    listing = items.reshape(top, rows).T
    listing = listing[jax.random.permutation(jax.random.fold_in(own, 1), rows)]
    turn = jax.random.randint(jax.random.fold_in(own, 2), (rows, 1), 0, top)
    return jnp.take_along_axis(listing, (jnp.arange(top)[None, :] + turn) % top, axis=1)


def portions_of(number_of, total, limit, lean, full):
    portions = [(1 << 20) // math.isqrt(grade ** lean) + 1 for grade in range(1, number_of + 1)]
    largest = limit if full else min(limit, max(-(-total // number_of), total * portions[0] // sum(portions)))
    least = 1 if total - largest >= number_of - 1 else 0
    given, rest = [largest] + [least] * (number_of - 1), total - largest - least * (number_of - 1)
    while rest > 0:
        movable = [i for i in range(1, number_of) if given[i] < largest] or [i for i in range(1, number_of) if given[i] < limit]
        whole, remaining = sum([portions[i] for i in movable]), rest
        for i in movable:
            addition = min(limit - given[i], max(1, remaining * portions[i] // whole), rest)
            given[i] = given[i] + addition
            rest = rest - addition
    return np.array(given)


def normal_values(key, shape, width, reach, pieces=(), held_as=jnp.bfloat16):
    entries = width * jax.random.normal(key, shape, jnp.float32)
    if pieces:
        entries = entries * shard_levels(key, shape, pieces, -0.22, 0.18)
    return jnp.clip(entries, -reach, reach).astype(held_as)


def setup_inputs(seed: int = 0, part: int = 0) -> dict:
    key_list = jax.random.split(jax.random.key(seed), 15)
    part_splits = jax.random.split(jax.random.fold_in(key_list[14], part), 15)
    queries = draw_queries(jax.random.fold_in(jax.random.fold_in(key_list[14], part), 71), part)
    token_keys = normal_values(part_splits[1], (SEQUENCE_TOTAL, KEY_VALUE_HEADS * HEAD_WIDTH), 1.0, 6.0, ((0, 32),))
    token_values = normal_values(part_splits[2], (SEQUENCE_TOTAL, KEY_VALUE_HEADS * HEAD_WIDTH), 1.0, 6.0, ((0, 32),))
    stored_keys = draw_stored_keys(jax.random.fold_in(jax.random.fold_in(key_list[14], part), 71), part)
    stored_values = normal_values(part_splits[4], (SEQUENCE_TOTAL, CACHE_POSITIONS, KEY_VALUE_HEADS * HEAD_WIDTH), 1.0, 6.0, ((0, 32),))
    kv_len = draw_kv_len(jax.random.fold_in(jax.random.fold_in(key_list[14], part), 71), part)
    residual = normal_values(part_splits[6], (SEQUENCE_TOTAL, D), 1.0, 6.0, ((0, 32),))
    out_weight = normal_values(key_list[7], (QUERY_HEADS * HEAD_WIDTH, D), (QUERY_HEADS * HEAD_WIDTH // 8) ** -0.5, 0.1875, ((0, 32),))
    norm_gain = jnp.clip(1.0 + 0.15 * jax.random.normal(key_list[8], (D,), jnp.float32), 0.25, 1.75).astype(jnp.bfloat16)
    expert_ids_keys = jax.random.split(jax.random.fold_in(part_splits[9], 1), SEQUENCE_TOTAL // (N_REPLICA * SEQ_DEV))
    expert_ids_turns = jax.random.permutation(jax.random.fold_in(part_splits[9], 3), SEQUENCE_TOTAL // (N_REPLICA * SEQ_DEV))
    expert_ids = jax.vmap(lambda own, number: shared_out(jax.random.fold_in(part_splits[9], 2), own, number, N_REPLICA * SEQ_DEV, EXPERTS, TOPK, MOST, 2))(expert_ids_keys, expert_ids_turns).reshape((SEQUENCE_TOTAL, TOPK))
    route_weight = jnp.clip(jnp.exp(math.log(1.0) - 2.9957323 * jax.random.uniform(part_splits[10], (SEQUENCE_TOTAL, TOPK), jnp.float32) ** shard_levels(part_splits[10], (SEQUENCE_TOTAL, TOPK), ((0, 16),), -0.2, 0.2)), 0.05, 1.0)
    w_gate = normal_values(key_list[11], (EXPERTS, D, FF), D ** -0.5, 0.09375, ((0, 16), (2, 2)))
    w_up = normal_values(key_list[12], (EXPERTS, D, FF), D ** -0.5, 0.09375, ((0, 16), (2, 2)))
    w_down = normal_values(key_list[13], (EXPERTS, FF, D), (FF // 4) ** -0.5, 0.4375, ((0, 16), (1, 2)))
    return dict(queries=queries, token_keys=token_keys, token_values=token_values, stored_keys=stored_keys, stored_values=stored_values, kv_len=kv_len, residual=residual, out_weight=out_weight, norm_gain=norm_gain, expert_ids=expert_ids, route_weight=route_weight, w_gate=w_gate, w_up=w_up, w_down=w_down)


def attend(queries, token_keys, token_values, stored_keys, stored_values, kv_len):
    sequence_rows = queries.shape[0]
    query_group_width = QUERY_HEADS // KEY_VALUE_HEADS
    query_head_rows = queries.astype(jnp.float32).reshape(sequence_rows, KEY_VALUE_HEADS, query_group_width, HEAD_WIDTH)
    keys_from_cache = stored_keys.astype(jnp.float32).reshape(sequence_rows, CACHE_POSITIONS, KEY_VALUE_HEADS, HEAD_WIDTH)
    values_from_cache = stored_values.astype(jnp.float32).reshape(sequence_rows, CACHE_POSITIONS, KEY_VALUE_HEADS, HEAD_WIDTH)
    keys_latest = token_keys.astype(jnp.float32).reshape(sequence_rows, KEY_VALUE_HEADS, HEAD_WIDTH)
    values_latest = token_values.astype(jnp.float32).reshape(sequence_rows, KEY_VALUE_HEADS, HEAD_WIDTH)
    inv_root = 1.0 / math.sqrt(HEAD_WIDTH)
    cached_scores = jnp.einsum('bgqd,bpgd->bgqp', query_head_rows, keys_from_cache) * inv_root
    positions = jnp.arange(CACHE_POSITIONS, dtype=jnp.int32)
    visible = positions[None, :] < kv_len[:, None]
    cached_scores = jnp.where(visible[:, None, None, :], cached_scores, -jnp.inf)
    fresh_score = jnp.einsum('bgqd,bgd->bgq', query_head_rows, keys_latest) * inv_root
    highest = jnp.maximum(lax.optimization_barrier(jnp.max(cached_scores, axis=-1)), fresh_score)
    cached_exp = jnp.exp(cached_scores - highest[..., None])
    fresh_exp = jnp.exp(fresh_score - highest)
    totals = lax.optimization_barrier(jnp.sum(cached_exp, axis=-1)) + fresh_exp
    cached_prob = lax.optimization_barrier((cached_exp / totals[..., None]).astype(jnp.bfloat16)).astype(jnp.float32)
    fresh_prob = lax.optimization_barrier((fresh_exp / totals).astype(jnp.bfloat16)).astype(jnp.float32)
    mixed = jnp.einsum('bgqp,bpgd->bgqd', cached_prob, values_from_cache)
    mixed = mixed + fresh_prob[..., None] * values_latest[:, :, None, :]
    return mixed.reshape(sequence_rows, QUERY_HEADS * HEAD_WIDTH).astype(jnp.bfloat16)

def reference(queries, token_keys, token_values, stored_keys, stored_values, kv_len, residual, out_weight, norm_gain, expert_ids, route_weight, w_gate, w_up, w_down):
    attended = attend(queries, token_keys, token_values, stored_keys, stored_values, kv_len)
    hidden_state = residual.astype(jnp.float32) + jnp.dot(attended, out_weight, preferred_element_type=jnp.float32)
    mean_square = lax.optimization_barrier(jnp.mean(hidden_state * hidden_state, axis=-1, keepdims=True))
    normed = (hidden_state * lax.rsqrt(mean_square + 1e-06) * norm_gain.astype(jnp.float32)).astype(jnp.bfloat16)
    mixing = route_weight / lax.optimization_barrier(jnp.sum(route_weight, axis=1, keepdims=True))
    flat_ids = expert_ids.reshape(-1).astype(jnp.int32)
    row_total = flat_ids.shape[0]
    sorted_rows = jnp.argsort(flat_ids, stable=True).astype(jnp.int32)
    member = flat_ids[None, :] == jnp.arange(EXPERTS, dtype=jnp.int32)[:, None]
    counts = lax.optimization_barrier(jnp.sum(member.astype(jnp.int32), axis=1)).astype(jnp.int32)
    starts = (jnp.cumsum(counts) - counts).astype(jnp.int32)
    capacity = MOST * N_EXPERT

    def one_expert(expert):
        offsets = jnp.arange(capacity, dtype=jnp.int32)
        taken_rows = sorted_rows[jnp.clip(starts[expert] + offsets, 0, row_total - 1)]
        alive_slot = offsets < counts[expert]
        inputs = normed[taken_rows // TOPK]
        gate_act = jnp.dot(inputs, w_gate[expert], preferred_element_type=jnp.float32)
        up_act = jnp.dot(inputs, w_up[expert], preferred_element_type=jnp.float32)
        hidden_act = (jax.nn.silu(gate_act) * up_act).astype(jnp.bfloat16)
        output = jnp.dot(hidden_act, w_down[expert], preferred_element_type=jnp.float32)
        return (jnp.where(alive_slot[:, None], output, 0.0), taken_rows)
    outputs, taken_all = lax.map(one_expert, jnp.arange(EXPERTS, dtype=jnp.int32))
    weights = mixing.reshape(-1)[taken_all]
    moe_out = jnp.zeros((SEQUENCE_TOTAL, D), jnp.float32).at[(taken_all // TOPK).reshape(-1)].add((weights[..., None] * outputs).reshape(-1, D))
    return (hidden_state + moe_out).astype(jnp.bfloat16)
```

```python
import functools
import math

import jax
import jax.numpy as jnp
from jax import lax
from jax.experimental import pallas as pl
from jax.experimental.pallas import tpu as pltpu
from jax.sharding import PartitionSpec as P

HEAD_WIDTH = 128
TILE = 16
MESH = pl.DeviceIdType.MESH
F32 = jnp.float32
BF16 = jnp.bfloat16


def regroup(outer, inner, back=False):
    size = 8 * outer * inner
    shape = (8 * TILE, size) if back else (size, 8 * TILE)
    a = lax.broadcasted_iota(jnp.int32, shape, 1 if back else 0)
    b = lax.broadcasted_iota(jnp.int32, shape, 0 if back else 1)
    o = a // (8 * inner)
    j = (a // inner) % 8
    i = a % inner
    return jnp.where(b == j * TILE + o * inner + i, 1.0, 0.0).astype(BF16)


def dot(a, b):
    return jnp.dot(a, b, preferred_element_type=F32)


def kernel(
    E, cap,
    q_ref, tk_ref, tv_ref, kv_ref, res_ref, gain_ref, ids_ref, rw_ref,
    k_hbm, v_hbm, ow_hbm, wg_hbm, wu_hbm, wd_hbm,
    out_ref,
    kb, vb, ow, wg, wu, wd,
    qs, tks, tvs, att, ratt, asm, yb, rs, resb, resp, hs, ssb, ssp,
    tts, whi, wlo, xb, xr, xs, hid, os, zb, zr, ub, up_,
    lsem, wsem, psend, precv, s1, r1, s2, r2, s3, r3, s4, r4,
):
    N = 2 * E
    e_me = lax.axis_index("expert")
    c = lax.axis_index("replica")
    rank = e_me * 2 + c
    S = q_ref.shape[0]
    T = 2 * S
    heads = q_ref.shape[1] // HEAD_WIDTH
    G = tk_ref.shape[1] // HEAD_WIDTH
    width = heads // G
    L = k_hbm.shape[1]
    D = res_ref.shape[1]
    half = D // 2
    hpc = heads // E
    Q = TILE // cap
    cw = half // Q
    mine = pl.ds(pl.multiple_of(c * half, half), half)
    other = pl.ds(pl.multiple_of((1 - c) * half, half), half)
    partner = {"expert": e_me, "replica": 1 - c}

    barrier = pltpu.get_barrier_semaphore()

    @pl.loop(1, N)
    def _(i):
        peer = lax.rem(rank + i, N)
        pl.semaphore_signal(
            barrier, inc=1,
            device_id={"expert": peer // 2, "replica": lax.rem(peer, 2)}, device_id_type=MESH,
        )

    kcopies = []
    for b in range(S):
        kcopies.append(pltpu.make_async_copy(k_hbm.at[b], kb.at[pl.ds(b * L, L)], lsem.at[b]))
    vcopies = []
    for b in range(S):
        vcopies.append(pltpu.make_async_copy(v_hbm.at[b], vb.at[pl.ds(b * L, L)], lsem.at[S + b]))
    for cp in kcopies + vcopies:
        cp.start()
    orow = ow_hbm.shape[0]
    drow = wd_hbm.shape[1]
    omine = pl.ds(pl.multiple_of(c * orow, orow), orow)
    dmine = pl.ds(pl.multiple_of(c * drow, drow), drow)
    wcopies = [
        pltpu.make_async_copy(ow_hbm.at[:, mine], ow.at[omine], wsem.at[0]),
        pltpu.make_async_copy(wg_hbm.at[0], wg, wsem.at[1]),
        pltpu.make_async_copy(wu_hbm.at[0], wu, wsem.at[2]),
        pltpu.make_async_copy(wd_hbm.at[0, :, mine], wd.at[dmine], wsem.at[3]),
    ]
    for cp in wcopies:
        cp.start()

    qf = q_ref[...].astype(F32)
    for h in range(heads):
        qs[pl.ds(S * h, S), :] = qf[:, h * HEAD_WIDTH:(h + 1) * HEAD_WIDTH]
    for rep in range(8 // S):
        tks[pl.ds(rep * S, S), :] = tk_ref[...].astype(F32)
        tvs[pl.ds(rep * S, S), :] = tv_ref[...].astype(F32)
        resb[pl.ds(rep * S, S), :] = res_ref[...].astype(F32)
    rows = S * width
    row = lax.broadcasted_iota(jnp.int32, (rows, S * L), 0)
    col = lax.broadcasted_iota(jnp.int32, (rows, S * L), 1)
    seq = col // L
    length = jnp.zeros((rows, S * L), jnp.int32)
    for b in range(S):
        length = jnp.where(seq == b, kv_ref[b], length)
    seen = (row % S == seq) & (col - seq * L < length)
    inv_root = 1.0 / math.sqrt(HEAD_WIDTH)
    for cp in kcopies + vcopies:
        cp.wait()
    for g in range(G):
        lanes = slice(g * HEAD_WIDTH, (g + 1) * HEAD_WIDTH)
        qg = qs[g * rows:(g + 1) * rows, :]
        score = lax.dot_general(
            qg.astype(BF16), kb[:, lanes], (((1,), (1,)), ((), ())), preferred_element_type=F32
        ) * inv_root
        score = jnp.where(seen, score, -jnp.inf)
        tk = tks[:, lanes]
        tv = tvs[:, lanes]
        fresh = jnp.sum(
            (qg.reshape(rows // 8, 8, HEAD_WIDTH) * tk[None]).reshape(rows, HEAD_WIDTH),
            axis=1, keepdims=True,
        ) * inv_root
        top = jnp.maximum(jnp.max(score, axis=1, keepdims=True), fresh)
        ex = jnp.exp(score - top)
        fex = jnp.exp(fresh - top)
        inv = 1.0 / (jnp.sum(ex, axis=1, keepdims=True) + fex)
        prob = (ex * inv).astype(BF16)
        fprob = (fex * inv).astype(BF16).astype(F32)
        o = dot(prob, vb[:, lanes])
        o = o + (
            fprob.reshape(rows // 8, 8, 1) * tv[None]
        ).reshape(rows, HEAD_WIDTH)
        per = hpc * S
        if per == TILE:
            att[g * rows:(g + 1) * rows, :] = o.astype(BF16)
        else:
            for j in range(rows // per):
                base = (g * (rows // per) + j) * TILE
                att[base:base + per, :] = o[j * per:(j + 1) * per].astype(BF16)

    pl.semaphore_wait(barrier, N - 1)

    def tile(ref, index):
        return ref.at[pl.ds(pl.multiple_of(index * TILE, TILE), TILE)]

    def att_copy(i, inbound=False):
        peer = lax.rem(rank + N - i, N) if inbound else lax.rem(rank + i, N)
        who = peer if inbound else rank
        return pltpu.make_async_remote_copy(
            src_ref=tile(att, peer // 2), dst_ref=tile(ratt, who),
            send_sem=s1.at[i], recv_sem=r1.at[who],
            device_id={"expert": peer // 2, "replica": lax.rem(peer, 2)}, device_id_type=MESH,
        )

    def spread(src, dst, send, recv, i, inbound=False):
        peer = lax.rem(e_me + E - i, E) if inbound else lax.rem(e_me + i, E)
        who = peer if inbound else e_me
        return pltpu.make_async_remote_copy(
            src_ref=tile(src, peer), dst_ref=tile(dst, who),
            send_sem=send.at[i], recv_sem=recv.at[who],
            device_id={"expert": peer, "replica": c}, device_id_type=MESH,
        )

    def beside(src, dst, k):
        return pltpu.make_async_remote_copy(
            src_ref=src, dst_ref=dst, send_sem=psend.at[k], recv_sem=precv.at[k],
            device_id=partner, device_id_type=MESH,
        )

    ow_x = beside(ow_hbm.at[:, other], ow.at[omine], 0)
    wd_x = beside(wd_hbm.at[0, :, other], wd.at[dmine], 1)
    res_x = beside(resb.at[:, other], resp, 2)
    ow_x.start()

    @pl.loop(1, N)
    def _(i):
        att_copy(i).start()

    own1 = pltpu.make_async_copy(tile(att, e_me), tile(ratt, rank), lsem.at[0])
    own1.start()
    res_x.start()
    wd_x.start()

    lanes_all = E * TILE
    lane = lax.broadcasted_iota(jnp.int32, (T, lanes_all), 1)
    tok = lax.broadcasted_iota(jnp.int32, (T, lanes_all), 0)
    le = lane // TILE
    lq = (lane // cap) % Q
    ls = lane % cap
    ids = ids_ref[...]
    rw = rw_ref[...]
    mix = rw / jnp.sum(rw, axis=1, keepdims=True)
    named = jnp.zeros((T, lanes_all), F32)
    weight = jnp.zeros((T, lanes_all), F32)
    for k in range(ids.shape[1]):
        hit = ids[:, k:k + 1] == le
        named = named + jnp.where(hit, 1.0, 0.0)
        weight = weight + jnp.where(hit, mix[:, k:k + 1], 0.0)
    before = jnp.zeros((T, lanes_all), F32)
    for t in range(T - 1):
        before = before + jnp.where(tok > t, named[t:t + 1, :], 0.0)
    chosen = jnp.where(before == ls.astype(F32), named, 0.0)
    weight = weight * chosen
    high = weight.astype(BF16).astype(F32)
    low = weight - high
    for p in range(Q):
        here = lq == p
        tts[p * T:(p + 1) * T, :] = jnp.where(here, chosen, 0.0)
        whi[p * T:(p + 1) * T, :] = jnp.where(here, high, 0.0)
        wlo[p * T:(p + 1) * T, :] = jnp.where(here, low, 0.0)

    wcopies[0].wait()
    ow_x.wait()
    own1.wait()

    @pl.loop(1, N)
    def _(i):
        att_copy(i, True).wait_recv()

    pa = regroup(hpc, S)
    for grp in range(N // 8):
        blk = dot(pa, ratt[grp * 8 * TILE:(grp + 1) * 8 * TILE, :]).astype(BF16)
        for h in range(hpc):
            asm[grp * 8 * S:(grp + 1) * 8 * S, h * HEAD_WIDTH:(h + 1) * HEAD_WIDTH] = (
                blk[h * 8 * S:(h + 1) * 8 * S]
            )
    quarter = half // 2
    step = min(512, quarter)
    for j in range(quarter // step):
        y0 = dot(asm[...], ow[:, j * step:(j + 1) * step])
        y1 = dot(asm[...], ow[:, quarter + j * step:quarter + (j + 1) * step])
        both = jnp.concatenate([y0.reshape(E, T, step), y1.reshape(E, T, step)], axis=1)
        yb[:, j * step:(j + 1) * step] = both.reshape(E * TILE, step).astype(BF16)

    @pl.loop(1, E)
    def _(i):
        spread(yb, rs, s2, r2, i).start()

    own2 = pltpu.make_async_copy(tile(yb, e_me), tile(rs, e_me), lsem.at[1])
    own2.start()
    res_x.wait()
    own2.wait()

    @pl.loop(1, E)
    def _(i):
        spread(yb, rs, s2, r2, i, True).wait_recv()

    total = rs[0:TILE, :].astype(F32)
    for j in range(1, E):
        total = total + rs[j * TILE:(j + 1) * TILE, :].astype(F32)
    projected = jnp.concatenate([total[:T], total[T:]], axis=1)
    trow = lax.broadcasted_iota(jnp.int32, (T, half), 0)
    own_token = trow // S == c
    hidden = jnp.where(own_token, resb[:, mine], resp[...]) + projected
    hs[...] = hidden
    square = jnp.sum(hidden * hidden, axis=1, keepdims=True)
    ssb[...] = jnp.broadcast_to(square, ssb.shape)
    ss_x = beside(ssb, ssp, 3)
    ss_x.start()
    scaled = hidden * gain_ref[:, mine].astype(F32)
    ss_x.wait()
    mean = (square + ssp[:, 0:1]) / D
    normed = scaled * lax.rsqrt(mean + 1e-06)
    stacked = jnp.concatenate([normed[:, p * cw:(p + 1) * cw] for p in range(Q)], axis=0)
    picked = lax.dot_general(
        tts[...].astype(BF16), stacked.astype(BF16), (((0,), (0,)), ((), ())),
        preferred_element_type=F32,
    )
    xb[...] = picked.astype(BF16)

    @pl.loop(1, E)
    def _(i):
        spread(xb, xr.at[c], s3, r3, i).start()

    own3 = pltpu.make_async_copy(tile(xb, e_me), tile(xr.at[c], e_me), lsem.at[2])
    own3.start()
    for cp in wcopies[1:]:
        cp.wait()
    wd_x.wait()
    own3.wait()

    @pl.loop(1, E)
    def _(i):
        spread(xb, xr.at[c], s3, r3, i, True).wait_recv()

    x_x = beside(xr.at[c], xr.at[c], 4)
    x_x.start()
    px = regroup(Q, cap)
    gc = 8 * cap
    gate = None
    for turn in range(2):
        side = c if turn == 0 else 1 - c
        if turn == 1:
            x_x.wait()
        for grp in range(E // 8):
            blk = dot(px, xr[side, grp * 8 * TILE:(grp + 1) * 8 * TILE, :]).astype(BF16)
            for p in range(Q):
                xs[turn, grp * gc:(grp + 1) * gc, p * cw:(p + 1) * cw] = blk[p * gc:(p + 1) * gc]
        feats = pl.ds(pl.multiple_of(side * half, half), half)
        gpart = dot(xs[turn], wg[feats, :])
        upart = dot(xs[turn], wu[feats, :])
        gate, up = (gpart, upart) if turn == 0 else (gate + gpart, up + upart)
    hid[c] = (gate / (1.0 + jnp.exp(-gate)) * up).astype(BF16)
    h_x = beside(hid.at[c], hid.at[c], 5)
    h_x.start()
    h_x.wait()
    for p in range(Q):
        cols = slice(p * cw, (p + 1) * cw)
        o = dot(hid[0], wd[0:drow, cols]) + dot(hid[1], wd[drow:2 * drow, cols])
        o = o.astype(BF16)
        for grp in range(E // 8):
            os[grp * 8 * TILE + p * gc:grp * 8 * TILE + (p + 1) * gc, :] = (
                o[grp * gc:(grp + 1) * gc]
            )
    pb = regroup(Q, cap, True)
    for grp in range(E // 8):
        part = slice(grp * 8 * TILE, (grp + 1) * 8 * TILE)
        zb[part, :] = dot(pb, os[part, :]).astype(BF16)

    @pl.loop(1, E)
    def _(i):
        spread(zb, zr, s4, r4, i).start()

    own4 = pltpu.make_async_copy(tile(zb, e_me), tile(zr, e_me), lsem.at[3])
    own4.start()
    own4.wait()

    @pl.loop(1, E)
    def _(i):
        spread(zb, zr, s4, r4, i, True).wait_recv()

    moe = dot(whi[...].astype(BF16), zr[...]) + dot(wlo[...].astype(BF16), zr[...])
    updated = hs[...] + jnp.concatenate([moe[p * T:(p + 1) * T] for p in range(Q)], axis=1)
    ub[...] = updated
    u_x = beside(ub, up_, 6)
    u_x.start()
    first = c == 0
    out_ref[:, mine] = jnp.where(first, updated[:S], updated[S:]).astype(BF16)
    u_x.wait()
    got = up_[...]
    out_ref[:, other] = jnp.where(first, got[:S], got[S:]).astype(BF16)

    @pl.loop(1, N)
    def _(i):
        att_copy(i).wait_send()

    @pl.loop(1, E)
    def _(i):
        spread(yb, rs, s2, r2, i).wait_send()
        spread(xb, xr.at[c], s3, r3, i).wait_send()
        spread(zb, zr, s4, r4, i).wait_send()


def on_device(
    queries, token_keys, token_values, stored_keys, stored_values, kv_len, residual, out_weight,
    norm_gain, expert_ids, route_weight, w_gate, w_up, w_down,
):
    E = lax.axis_size("expert")
    N = 2 * E
    S, features = queries.shape
    T = 2 * S
    L = stored_keys.shape[1]
    KW = token_keys.shape[1]
    D = residual.shape[1]
    half = D // 2
    topk = expert_ids.shape[1]
    FH = w_gate.shape[2]
    cap = max(2, -(-(T * topk) // E))
    Q = TILE // cap
    cw = half // Q
    orow = out_weight.shape[0]
    vmem = pl.BlockSpec(memory_space=pltpu.VMEM)
    smem = pl.BlockSpec(memory_space=pltpu.SMEM)
    hbm = pl.BlockSpec(memory_space=pl.ANY)
    V = pltpu.VMEM
    dma = pltpu.SemaphoreType.DMA
    scratch = [
        V((S * L, KW), BF16), V((S * L, KW), BF16),
        V((2 * orow, half), BF16), V((D, FH), BF16), V((D, FH), BF16), V((2 * FH, half), BF16),
        V((S * features // HEAD_WIDTH, HEAD_WIDTH), F32), V((8, KW), F32), V((8, KW), F32),
        V((E * TILE, HEAD_WIDTH), BF16), V((N * TILE, HEAD_WIDTH), BF16),
        V((N * S, 2 * orow), BF16),
        V((E * TILE, half // 2), BF16), V((E * TILE, half // 2), BF16),
        V((T, D), F32), V((T, half), F32), V((T, half), F32), V((T, 128), F32), V((T, 128), F32),
        V((Q * T, E * TILE), F32), V((Q * T, E * TILE), F32), V((Q * T, E * TILE), F32),
        V((E * TILE, cw), BF16), V((2, E * TILE, cw), BF16), V((2, E * cap, half), BF16),
        V((2, E * cap, FH), BF16),
        V((E * TILE, cw), BF16), V((E * TILE, cw), BF16), V((E * TILE, cw), BF16),
        V((T, half), F32), V((T, half), F32),
        dma((2 * S,)), dma((4,)), dma((7,)), dma((7,)),
        dma((N,)), dma((N,)), dma((E,)), dma((E,)), dma((E,)), dma((E,)), dma((E,)), dma((E,)),
    ]
    return pl.pallas_call(
        functools.partial(kernel, E, cap),
        out_shape=jax.ShapeDtypeStruct((S, D), BF16),
        in_specs=[vmem, vmem, vmem, smem, vmem, vmem, vmem, vmem, hbm, hbm, hbm, hbm, hbm, hbm],
        out_specs=vmem,
        scratch_shapes=scratch,
        compiler_params=pltpu.CompilerParams(
            collective_id=0, has_side_effects=True, vmem_limit_bytes=48 * 1024 * 1024
        ),
    )(
        queries, token_keys, token_values, kv_len, residual, norm_gain.reshape(1, D), expert_ids,
        route_weight, stored_keys, stored_values, out_weight, w_gate, w_up, w_down,
    )


def solution(mesh):
    rows = P(("groups", "expert", "replica"), None)
    cube = P(("groups", "expert", "replica"), None, None)
    in_specs = (
        rows, rows, rows, cube, cube, P(("groups", "expert", "replica")), rows,
        P(("expert", "replica"), None), P(), P(("groups", "expert"), None),
        P(("groups", "expert"), None), P("expert", None, "replica"),
        P("expert", None, "replica"), P("expert", "replica", None),
    )
    return jax.shard_map(
        on_device, mesh=mesh, in_specs=in_specs, out_specs=rows, check_vma=False
    )
```

```python
import functools
import math

import jax
import jax.numpy as jnp
from jax import lax
from jax.experimental import pallas as pl
from jax.experimental.pallas import tpu as pltpu
from jax.sharding import PartitionSpec as P

HEAD_WIDTH = 128
TILE = 16
CHUNKS = 1
MESH = pl.DeviceIdType.MESH
F32 = jnp.float32
BF16 = jnp.bfloat16


def regroup(outer, inner, back=False):
    size = 8 * outer * inner
    shape = (8 * TILE, size) if back else (size, 8 * TILE)
    a = lax.broadcasted_iota(jnp.int32, shape, 1 if back else 0)
    b = lax.broadcasted_iota(jnp.int32, shape, 0 if back else 1)
    o = a // (8 * inner)
    j = (a // inner) % 8
    i = a % inner
    return jnp.where(b == j * TILE + o * inner + i, 1.0, 0.0).astype(BF16)


def dot(a, b):
    return jnp.dot(a, b, preferred_element_type=F32)


def flipped(index, mask, bits):
    total = 0
    for k in range(bits):
        place = 1 << k
        total = total + lax.rem(lax.div(index, place) + lax.div(mask, place), 2) * place
    return total


def kernel(
    E, cap,
    q_hbm, tk_hbm, tv_hbm, kv_hbm, res_hbm, gain_hbm, ids_hbm, rw_hbm,
    k_hbm, v_hbm, ow_hbm, wg_hbm, wu_hbm, wd_hbm,
    out_ref,
    q_ref, tk_ref, tv_ref, kv_ref, res_ref, gain_ref, ids_ref, rw_ref,
    kb, vb, ow, wg, wu, wd,
    qs, tks, tvs, att, ratt, asm, yb, rs, resb, resp, hs, ssb, ssp,
    tts, whi, wlo, xb, xr, xs, hid, os, zb, zr, ub, up_,
    lsem, osem, wsem, isem, psend, precv, s1, r1, s2, r2, s3, r3, s4, r4,
):
    N = 2 * E
    e_me = lax.axis_index("expert")
    c = lax.axis_index("replica")
    rank = e_me * 2 + c
    S = q_ref.shape[0]
    T = 2 * S
    heads = q_ref.shape[1] // HEAD_WIDTH
    G = tk_ref.shape[1] // HEAD_WIDTH
    width = heads // G
    L = k_hbm.shape[1]
    D = res_ref.shape[1]
    half = D // 2
    hpc = heads // E
    Q = TILE // cap
    cw = half // Q
    mine = pl.ds(pl.multiple_of(c * half, half), half)
    other = pl.ds(pl.multiple_of((1 - c) * half, half), half)
    partner = {"expert": e_me, "replica": 1 - c}

    small = [
        pltpu.make_async_copy(src, dst, isem.at[k])
        for k, (src, dst) in enumerate((
            (q_hbm, q_ref), (tk_hbm, tk_ref), (tv_hbm, tv_ref), (kv_hbm, kv_ref),
            (res_hbm, res_ref), (gain_hbm, gain_ref), (ids_hbm, ids_ref), (rw_hbm, rw_ref),
        ))
    ]
    for cp in small:
        cp.start()
    barrier = pltpu.get_barrier_semaphore()

    @pl.loop(1, N)
    def _(i):
        peer = lax.rem(rank + i, N)
        pl.semaphore_signal(
            barrier, inc=1,
            device_id={"expert": peer // 2, "replica": lax.rem(peer, 2)}, device_id_type=MESH,
        )

    kcopies = []
    for b in range(S):
        kcopies.append(pltpu.make_async_copy(k_hbm.at[b], kb.at[pl.ds(b * L, L)], lsem.at[b]))
    vcopies = []
    for b in range(S):
        vcopies.append(pltpu.make_async_copy(v_hbm.at[b], vb.at[pl.ds(b * L, L)], lsem.at[S + b]))
    for cp in kcopies + vcopies:
        cp.start()
    orow = ow_hbm.shape[0]
    drow = wd_hbm.shape[1]
    omine = pl.ds(pl.multiple_of(c * orow, orow), orow)
    dmine = pl.ds(pl.multiple_of(c * drow, drow), drow)
    wcopies = [
        pltpu.make_async_copy(ow_hbm.at[:, mine], ow.at[omine], wsem.at[0]),
        pltpu.make_async_copy(wg_hbm.at[0], wg, wsem.at[1]),
        pltpu.make_async_copy(wu_hbm.at[0], wu, wsem.at[2]),
        pltpu.make_async_copy(wd_hbm.at[0, :, mine], wd.at[dmine], wsem.at[3]),
    ]
    for cp in wcopies:
        cp.start()

    for cp in small:
        cp.wait()
    qf = q_ref[...].astype(F32)
    for h in range(heads):
        qs[pl.ds(S * h, S), :] = qf[:, h * HEAD_WIDTH:(h + 1) * HEAD_WIDTH]
    for rep in range(8 // S):
        tks[pl.ds(rep * S, S), :] = tk_ref[...].astype(F32)
        tvs[pl.ds(rep * S, S), :] = tv_ref[...].astype(F32)
        resb[pl.ds(rep * S, S), :] = res_ref[...].astype(F32)
    rows = S * width
    row = lax.broadcasted_iota(jnp.int32, (rows, S * L), 0)
    col = lax.broadcasted_iota(jnp.int32, (rows, S * L), 1)
    seq = col // L
    length = jnp.zeros((rows, S * L), jnp.int32)
    for b in range(S):
        length = jnp.where(seq == b, kv_ref[b], length)
    seen = (row % S == seq) & (col - seq * L < length)
    inv_root = 1.0 / math.sqrt(HEAD_WIDTH)
    for cp in kcopies + vcopies:
        cp.wait()
    for g in range(G):
        lanes = slice(g * HEAD_WIDTH, (g + 1) * HEAD_WIDTH)
        qg = qs[g * rows:(g + 1) * rows, :]
        score = lax.dot_general(
            qg.astype(BF16), kb[:, lanes], (((1,), (1,)), ((), ())), preferred_element_type=F32
        ) * inv_root
        score = jnp.where(seen, score, -jnp.inf)
        tk = tks[:, lanes]
        tv = tvs[:, lanes]
        fresh = jnp.sum(
            (qg.reshape(rows // 8, 8, HEAD_WIDTH) * tk[None]).reshape(rows, HEAD_WIDTH),
            axis=1, keepdims=True,
        ) * inv_root
        top = jnp.maximum(jnp.max(score, axis=1, keepdims=True), fresh)
        ex = jnp.exp(score - top)
        fex = jnp.exp(fresh - top)
        inv = 1.0 / (jnp.sum(ex, axis=1, keepdims=True) + fex)
        prob = (ex * inv).astype(BF16)
        fprob = (fex * inv).astype(BF16).astype(F32)
        o = dot(prob, vb[:, lanes])
        o = o + (
            fprob.reshape(rows // 8, 8, 1) * tv[None]
        ).reshape(rows, HEAD_WIDTH)
        per = hpc * S
        if per == TILE:
            att[g * rows:(g + 1) * rows, :] = o.astype(BF16)
        else:
            for j in range(rows // per):
                base = (g * (rows // per) + j) * TILE
                att[base:base + per, :] = o[j * per:(j + 1) * per].astype(BF16)

    pl.semaphore_wait(barrier, N - 1)

    def tile(ref, index):
        return ref.at[pl.ds(pl.multiple_of(index * TILE, TILE), TILE)]

    def partner_of(index, i, count, inbound):
        if count & (count - 1) == 0:
            return flipped(index, count - i, count.bit_length() - 1)
        return lax.rem(index + count - i, count) if inbound else lax.rem(index + i, count)

    def att_copy(i, inbound=False):
        peer = partner_of(rank, i, N, inbound)
        who = peer if inbound else rank
        return pltpu.make_async_remote_copy(
            src_ref=tile(att, peer // 2), dst_ref=tile(ratt, who),
            send_sem=s1.at[i], recv_sem=r1.at[who],
            device_id={"expert": peer // 2, "replica": lax.rem(peer, 2)}, device_id_type=MESH,
        )

    def piece(ref, index, k):
        wide = ref.shape[-1] // CHUNKS
        return ref.at[
            pl.ds(pl.multiple_of(index * TILE, TILE), TILE), pl.ds(k * wide, wide)
        ]

    def spread(src, dst, send, recv, k, i, inbound=False):
        peer = partner_of(e_me, i, E, inbound)
        who = peer if inbound else e_me
        return pltpu.make_async_remote_copy(
            src_ref=piece(src, peer, k), dst_ref=piece(dst, who, k),
            send_sem=send.at[k, i], recv_sem=recv.at[k, who],
            device_id={"expert": peer, "replica": c}, device_id_type=MESH,
        )

    def scatter(src, dst, send, recv, k, own):
        @pl.loop(1, E)
        def _(i):
            spread(src, dst, send, recv, k, i).start()

        cp = pltpu.make_async_copy(piece(src, e_me, k), piece(dst, e_me, k), osem.at[own, k])
        cp.start()
        return cp

    def gather(src, dst, send, recv, k, cp):
        cp.wait()

        @pl.loop(1, E)
        def _(i):
            spread(src, dst, send, recv, k, i, True).wait_recv()

    def beside(src, dst, k):
        return pltpu.make_async_remote_copy(
            src_ref=src, dst_ref=dst, send_sem=psend.at[k], recv_sem=precv.at[k],
            device_id=partner, device_id_type=MESH,
        )

    ow_x = beside(ow_hbm.at[:, other], ow.at[omine], 0)
    wd_x = beside(wd_hbm.at[0, :, other], wd.at[dmine], 1)
    res_x = beside(resb.at[:, other], resp, 2)
    ow_x.start()

    @pl.loop(1, N)
    def _(i):
        att_copy(i).start()

    own1 = pltpu.make_async_copy(tile(att, e_me), tile(ratt, rank), lsem.at[0])
    own1.start()
    res_x.start()
    wd_x.start()

    lanes_all = E * TILE
    lane = lax.broadcasted_iota(jnp.int32, (T, lanes_all), 1)
    tok = lax.broadcasted_iota(jnp.int32, (T, lanes_all), 0)
    le = lane // TILE
    lq = (lane // cap) % Q
    ls = lane % cap
    ids = ids_ref[...]
    rw = rw_ref[...]
    mix = rw / jnp.sum(rw, axis=1, keepdims=True)
    named = jnp.zeros((T, lanes_all), F32)
    weight = jnp.zeros((T, lanes_all), F32)
    for k in range(ids.shape[1]):
        hit = ids[:, k:k + 1] == le
        named = named + jnp.where(hit, 1.0, 0.0)
        weight = weight + jnp.where(hit, mix[:, k:k + 1], 0.0)
    before = jnp.zeros((T, lanes_all), F32)
    for t in range(T - 1):
        before = before + jnp.where(tok > t, named[t:t + 1, :], 0.0)
    chosen = jnp.where(before == ls.astype(F32), named, 0.0)
    weight = weight * chosen
    high = weight.astype(BF16).astype(F32)
    low = weight - high
    for p in range(Q):
        here = lq == p
        tts[p * T:(p + 1) * T, :] = jnp.where(here, chosen, 0.0)
        whi[p * T:(p + 1) * T, :] = jnp.where(here, high, 0.0)
        wlo[p * T:(p + 1) * T, :] = jnp.where(here, low, 0.0)

    wcopies[0].wait()
    ow_x.wait()
    own1.wait()

    @pl.loop(1, N)
    def _(i):
        att_copy(i, True).wait_recv()

    pa = regroup(hpc, S)
    for grp in range(N // 8):
        blk = dot(pa, ratt[grp * 8 * TILE:(grp + 1) * 8 * TILE, :]).astype(BF16)
        for h in range(hpc):
            asm[grp * 8 * S:(grp + 1) * 8 * S, h * HEAD_WIDTH:(h + 1) * HEAD_WIDTH] = (
                blk[h * 8 * S:(h + 1) * 8 * S]
            )
    quarter = half // 2
    step = quarter // CHUNKS
    own2 = []
    for j in range(CHUNKS):
        y0 = dot(asm[...], ow[:, j * step:(j + 1) * step])
        y1 = dot(asm[...], ow[:, quarter + j * step:quarter + (j + 1) * step])
        both = jnp.concatenate([y0.reshape(E, T, step), y1.reshape(E, T, step)], axis=1)
        yb[:, j * step:(j + 1) * step] = both.reshape(E * TILE, step).astype(BF16)
        own2.append(scatter(yb, rs, s2, r2, j, 0))
    res_x.wait()
    sums = []
    for j in range(CHUNKS):
        gather(yb, rs, s2, r2, j, own2[j])
        cols = slice(j * step, (j + 1) * step)
        total = rs[0:TILE, cols].astype(F32)
        for k in range(1, E):
            total = total + rs[k * TILE:(k + 1) * TILE, cols].astype(F32)
        sums.append(total)
    projected = jnp.concatenate([t[:T] for t in sums] + [t[T:] for t in sums], axis=1)
    trow = lax.broadcasted_iota(jnp.int32, (T, half), 0)
    own_token = trow // S == c
    hidden = jnp.where(own_token, resb[:, mine], resp[...]) + projected
    hs[...] = hidden
    square = jnp.sum(hidden * hidden, axis=1, keepdims=True)
    ssb[...] = jnp.broadcast_to(square, ssb.shape)
    ss_x = beside(ssb, ssp, 3)
    ss_x.start()
    scaled = hidden * gain_ref[mine].astype(F32).reshape(1, half)
    ss_x.wait()
    mean = (square + ssp[:, 0:1]) / D
    normed = scaled * lax.rsqrt(mean + 1e-06)
    stacked = jnp.concatenate([normed[:, p * cw:(p + 1) * cw] for p in range(Q)], axis=0)
    stacked = stacked.astype(BF16)
    table = tts[...].astype(BF16)
    wide = cw // CHUNKS
    own3 = []
    for k in range(CHUNKS):
        picked = lax.dot_general(
            table, stacked[:, k * wide:(k + 1) * wide], (((0,), (0,)), ((), ())),
            preferred_element_type=F32,
        )
        xb[:, k * wide:(k + 1) * wide] = picked.astype(BF16)
        own3.append(scatter(xb, xr.at[c], s3, r3, k, 1))
    for cp in wcopies[1:]:
        cp.wait()
    wd_x.wait()
    px = regroup(Q, cap)
    gc = 8 * cap
    gate = jnp.zeros((E * cap, wg.shape[1]), F32)
    up = gate
    forwards = []
    for turn in range(2):
        side = c if turn == 0 else 1 - c
        for k in range(CHUNKS):
            cols = slice(k * wide, (k + 1) * wide)
            if turn == 0:
                gather(xb, xr.at[c], s3, r3, k, own3[k])
                mid = xr.at[c, :, pl.ds(k * wide, wide)]
                forwards.append(beside(mid, mid, (4, 7)[k]))
                forwards[k].start()
            else:
                forwards[k].wait()
            for grp in range(E // 8):
                blk = dot(px, xr[side, grp * 8 * TILE:(grp + 1) * 8 * TILE, cols]).astype(BF16)
                for p in range(Q):
                    xs[turn, grp * gc:(grp + 1) * gc, p * cw + k * wide:p * cw + (k + 1) * wide] = (
                        blk[p * gc:(p + 1) * gc]
                    )
            for p in range(Q):
                start = p * cw + k * wide
                feats = pl.ds(pl.multiple_of(side * half + start, wide), wide)
                rows_in = xs[turn, :, start:start + wide]
                gate = gate + dot(rows_in, wg[feats, :])
                up = up + dot(rows_in, wu[feats, :])
    hid[c] = (gate / (1.0 + jnp.exp(-gate)) * up).astype(BF16)
    h_x = beside(hid.at[c], hid.at[c], 5)
    h_x.start()
    h_x.wait()
    pb = regroup(Q, cap, True)
    own4 = []
    for k in range(CHUNKS):
        mid = slice(k * wide, (k + 1) * wide)
        for p in range(Q):
            cols = slice(p * cw + k * wide, p * cw + (k + 1) * wide)
            o = dot(hid[0], wd[0:drow, cols]) + dot(hid[1], wd[drow:2 * drow, cols])
            o = o.astype(BF16)
            for grp in range(E // 8):
                os[grp * 8 * TILE + p * gc:grp * 8 * TILE + (p + 1) * gc, mid] = (
                    o[grp * gc:(grp + 1) * gc]
                )
        for grp in range(E // 8):
            part = slice(grp * 8 * TILE, (grp + 1) * 8 * TILE)
            zb[part, mid] = dot(pb, os[part, mid]).astype(BF16)
        own4.append(scatter(zb, zr, s4, r4, k, 2))
    parts = []
    for k in range(CHUNKS):
        mid = slice(k * wide, (k + 1) * wide)
        gather(zb, zr, s4, r4, k, own4[k])
        parts.append(
            dot(whi[...].astype(BF16), zr[:, mid]) + dot(wlo[...].astype(BF16), zr[:, mid])
        )
    moe = jnp.concatenate(parts, axis=1)
    updated = hs[...] + jnp.concatenate([moe[p * T:(p + 1) * T] for p in range(Q)], axis=1)
    ub[...] = updated
    u_x = beside(ub, up_, 6)
    u_x.start()
    first = c == 0
    out_ref[:, mine] = jnp.where(first, updated[:S], updated[S:]).astype(BF16)
    u_x.wait()
    got = up_[...]
    out_ref[:, other] = jnp.where(first, got[:S], got[S:]).astype(BF16)

    @pl.loop(1, N)
    def _(i):
        att_copy(i).wait_send()

    @pl.loop(1, E)
    def _(i):
        for k in range(CHUNKS):
            spread(yb, rs, s2, r2, k, i).wait_send()
            spread(xb, xr.at[c], s3, r3, k, i).wait_send()
            spread(zb, zr, s4, r4, k, i).wait_send()


def on_device(
    queries, token_keys, token_values, stored_keys, stored_values, kv_len, residual, out_weight,
    norm_gain, expert_ids, route_weight, w_gate, w_up, w_down,
):
    E = lax.axis_size("expert")
    N = 2 * E
    S, features = queries.shape
    T = 2 * S
    L = stored_keys.shape[1]
    KW = token_keys.shape[1]
    D = residual.shape[1]
    half = D // 2
    topk = expert_ids.shape[1]
    FH = w_gate.shape[2]
    cap = max(2, -(-(T * topk) // E))
    Q = TILE // cap
    cw = half // Q
    orow = out_weight.shape[0]
    vmem = pl.BlockSpec(memory_space=pltpu.VMEM)
    hbm = pl.BlockSpec(memory_space=pltpu.HBM)
    V = pltpu.VMEM
    dma = pltpu.SemaphoreType.DMA
    scratch = [
        V((S, features), BF16), V((S, KW), BF16), V((S, KW), BF16), pltpu.SMEM((S,), jnp.int32),
        V((S, D), BF16), V((D,), BF16), V(expert_ids.shape, jnp.int32), V(route_weight.shape, F32),
        V((S * L, KW), BF16), V((S * L, KW), BF16),
        V((2 * orow, half), BF16), V((D, FH), BF16), V((D, FH), BF16), V((2 * FH, half), BF16),
        V((S * features // HEAD_WIDTH, HEAD_WIDTH), F32), V((8, KW), F32), V((8, KW), F32),
        V((E * TILE, HEAD_WIDTH), BF16), V((N * TILE, HEAD_WIDTH), BF16),
        V((N * S, 2 * orow), BF16),
        V((E * TILE, half // 2), BF16), V((E * TILE, half // 2), BF16),
        V((T, D), F32), V((T, half), F32), V((T, half), F32), V((T, 128), F32), V((T, 128), F32),
        V((Q * T, E * TILE), F32), V((Q * T, E * TILE), F32), V((Q * T, E * TILE), F32),
        V((E * TILE, cw), BF16), V((2, E * TILE, cw), BF16), V((2, E * cap, half), BF16),
        V((2, E * cap, FH), BF16),
        V((E * TILE, cw), BF16), V((E * TILE, cw), BF16), V((E * TILE, cw), BF16),
        V((T, half), F32), V((T, half), F32),
        dma((2 * S,)), dma((3, CHUNKS)), dma((4,)), dma((8,)), dma((8,)), dma((8,)),
        dma((N,)), dma((N,)), *[dma((CHUNKS, E))] * 6,
    ]
    return pl.pallas_call(
        functools.partial(kernel, E, cap),
        out_shape=jax.ShapeDtypeStruct((S, D), BF16),
        in_specs=[hbm] * 14,
        out_specs=vmem,
        scratch_shapes=scratch,
        compiler_params=pltpu.CompilerParams(
            collective_id=0, has_side_effects=True, vmem_limit_bytes=67043328
        ),
    )(
        queries, token_keys, token_values, kv_len, residual, norm_gain, expert_ids,
        route_weight, stored_keys, stored_values, out_weight, w_gate, w_up, w_down,
    )


def solution(mesh):
    rows = P(("groups", "expert", "replica"), None)
    cube = P(("groups", "expert", "replica"), None, None)
    in_specs = (
        rows, rows, rows, cube, cube, P(("groups", "expert", "replica")), rows,
        P(("expert", "replica"), None), P(), P(("groups", "expert"), None),
        P(("groups", "expert"), None), P("expert", None, "replica"),
        P("expert", None, "replica"), P("expert", "replica", None),
    )
    return jax.shard_map(
        on_device, mesh=mesh, in_specs=in_specs, out_specs=rows, check_vma=False
    )
```
